32 devices in a mesh: mode: 8 (over y, x, core), tm: 4 (over z).
Axes of the slice: x: 2, y: 2, z: 4, core: 2. Of those that a mesh axis runs over, the one named last changes fastest.
Arguments:
- field: float32 [2, 128, 65536], P(None, 'mode', 'tm'), may hold values from -1.8 to 1.8
- beta: float32 [3, 128], P(None, 'mode'), may hold values from -1 to 1
- quartets: int32 [4, 1024], replicated, may hold values from 0 to 127
- intersections: float32 [1024], replicated, may hold values from -0.12 to 0.12
Outputs:
- field_out: float32 [2, 128, 65536], P(None, 'mode', 'tm')
- errors: float32 [2, 128], P(None, 'mode')
The draws below stay inside these ranges and needn't reach their ends.
All inputs are finite; a program needn't handle non-finite values.
Results may differ from the reference program's by a relative error of at most 0.0003.
Values sent between devices are 32-bit elements; how exact they have to be, the bound alone decides.
A program may use at most 128 MiB of HBM per device.

```python
import math
import jax
import jax.numpy as jnp
from jax import lax

MODES = 128
TIME = 65536
STEPS = 2
QUARTETS = 1024


def draw_field(key, part):
    first_key = jax.random.fold_in(key, 0)
    ramp = lax.iota(jnp.float32, TIME) / TIME
    envelope = 0.6 * (1.0 + 2.0 * ramp)
    values = jnp.clip(0.5 * jax.random.normal(first_key, (2, MODES, TIME), jnp.float32), -1.0, 1.0)
    return (values * envelope).astype(jnp.float32)


def set_ends(array, key, low, top_value):
    shape = array.shape
    index_at = [jax.random.randint(jax.random.fold_in(key, axis), (), 0, shape[axis]) for axis in range(len(shape))]
    array = array.at[tuple(index_at)].set(low)
    longest = shape.index(max(shape))
    index_at[longest] = (index_at[longest] + 1) % shape[longest]
    return array.at[tuple(index_at)].set(top_value)


def block_levels(own_key, extent, cuts, low, largest):
    def one(position, shards_of):
        heights = jax.random.uniform(jax.random.fold_in(jax.random.fold_in(own_key, 6), position), (shards_of,), jnp.float32, low / len(cuts), largest / len(cuts))
        return jnp.repeat(jnp.exp(heights), extent[position] // shards_of).reshape((-1,) + (1,) * (len(extent) - position - 1))

    factor_of = one(*cuts[0])
    for cut in cuts[1:]:
        factor_of = factor_of * one(*cut)
    return factor_of


def bell_draw(rng, dims, scale, reach, dtype=jnp.bfloat16):
    return jnp.clip(scale * jax.random.normal(rng, dims, jnp.float32), -reach, reach).astype(dtype)


def setup_inputs(seed: int = 0) -> dict:
    seeds = jax.random.split(jax.random.key(seed), 5)
    return {
        "field": draw_field(jax.random.fold_in(seeds[4], 71), 0),
        "beta": jnp.clip(jax.random.uniform(seeds[1], (3, MODES), jnp.float32, -1.0, 1.0) * block_levels(seeds[1], (3, MODES), ((1, 8),), -0.4, 0.0), -1.0, 1.0),
        "quartets": set_ends(jax.random.randint(seeds[2], (4, QUARTETS), 0, MODES), jax.random.fold_in(seeds[2], 1), 0, MODES - 1).astype(jnp.int32),
        "intersections": bell_draw(seeds[3], (QUARTETS,), 0.03, 0.12, jnp.float32),
    }


epsilon = 1e-06

def phase_of(offset, slope, curve, frequency):
    return math.pi * offset + 300.0 * slope * frequency + 3000.0 * curve * frequency * frequency

def triple_product(left_field, middle_field, conj_field):
    prod_re = left_field[0] * middle_field[0] - left_field[1] * middle_field[1]
    prod_im = left_field[0] * middle_field[1] + left_field[1] * middle_field[0]
    out_re = prod_re * conj_field[0] + prod_im * conj_field[1]
    out_im = prod_im * conj_field[0] - prod_re * conj_field[1]
    return (out_re, out_im)

def kerr_term(fields, quartets, intersections):
    blocks = quartets.shape[1] // 128
    grouped = quartets.reshape(4, blocks, 128).transpose(1, 0, 2)
    weights = intersections.reshape(blocks, 128)

    def accumulate(running, block_item):
        indices, weight = block_item
        out_re, out_im = triple_product(fields[:, indices[1], :], fields[:, indices[2], :], fields[:, indices[3], :])
        contrib = jnp.stack([weight[:, None] * -out_im, weight[:, None] * out_re])
        return (running.at[:, indices[0], :].add(contrib), None)
    running, unused = lax.scan(accumulate, jnp.zeros_like(fields), (grouped, weights))
    return running

def reference(field, beta, quartets, intersections):
    sample_index = lax.iota(jnp.int32, TIME)
    signed = jnp.where(sample_index < TIME // 2, sample_index, sample_index - TIME)
    frequency = signed.astype(jnp.float32) / (TIME / 2)
    angle = phase_of(beta[0][:, None], beta[1][:, None], beta[2][:, None], frequency[None, :])
    rotor = lax.complex(jnp.cos(angle), jnp.sin(angle))
    error_rows = []
    for step_index in range(STEPS):
        spectrum = jnp.fft.fft(lax.complex(field[0], field[1]), axis=-1) * rotor
        moved = jnp.fft.ifft(spectrum, axis=-1)
        linear = jnp.stack([jnp.real(moved), jnp.imag(moved)])
        first = kerr_term(linear, quartets, intersections)
        second = kerr_term(linear + first, quartets, intersections)
        field = linear + 0.5 * (first + second)
        estimate = 0.5 * (second - first)
        error_sq = lax.optimization_barrier(jnp.sum(estimate * estimate, axis=(0, 2)))
        field_sq = lax.optimization_barrier(jnp.sum(field * field, axis=(0, 2)))
        error_rows.append(jnp.sqrt(error_sq / (field_sq + epsilon)))
    return (field, jnp.stack(error_rows))
```

```python
import functools
import math

import jax
import jax.numpy as jnp
from jax import lax
from jax.experimental import pallas as pl
from jax.experimental.pallas import tpu as pltpu
from jax.sharding import PartitionSpec as P

RADIX = 256
STEPS = 2


epsilon = 1e-06


def phase_of(offset, slope, curve, frequency):
    return math.pi * offset + 300.0 * slope * frequency + 3000.0 * curve * frequency * frequency


def triple_product(left_field, middle_field, conj_field):
    prod_re = left_field[0] * middle_field[0] - left_field[1] * middle_field[1]
    prod_im = left_field[0] * middle_field[1] + left_field[1] * middle_field[0]
    out_re = prod_re * conj_field[0] + prod_im * conj_field[1]
    out_im = prod_im * conj_field[0] - prod_re * conj_field[1]
    return (out_re, out_im)


def contract(form, first_operand, second_operand):
    return jnp.einsum(form, first_operand, second_operand, precision=lax.Precision.HIGHEST)


def rotate(real_part, imag_part, angle):
    cosine = jnp.cos(angle)
    sine_part = jnp.sin(angle)
    return (real_part * cosine - imag_part * sine_part, real_part * sine_part + imag_part * cosine)


def dft_tables(length):
    positions = lax.iota(jnp.int32, length)
    product = positions[:, None] * positions[None, :] % length
    angle = -2.0 * math.pi / length * product.astype(jnp.float32)
    return (jnp.cos(angle), jnp.sin(angle))


def to_columns(state):
    return lax.all_to_all(state, "tm", split_axis=3, concat_axis=2, tiled=True)


def to_rows(state):
    return lax.all_to_all(state, "tm", split_axis=2, concat_axis=3, tiled=True)


def linear_step(state, beta, table_re, table_im):
    radix_size = table_re.shape[0]
    total_time = radix_size * radix_size
    cols_local = state.shape[3]
    tm_index = lax.axis_index("tm")
    head_re = contract("ka,mab->mkb", table_re, state[0]) - contract(
        "ka,mab->mkb", table_im, state[1]
    )
    head_im = contract("ka,mab->mkb", table_re, state[1]) + contract(
        "ka,mab->mkb", table_im, state[0]
    )
    column = tm_index * cols_local + lax.iota(jnp.int32, cols_local)
    row_position = lax.iota(jnp.int32, radix_size)
    twist = (
        -2.0
        * math.pi
        / total_time
        * (row_position[:, None] * column[None, :] % total_time).astype(jnp.float32)
    )
    head_re, head_im = rotate(head_re, head_im, twist[None])
    turned = lax.all_to_all(
        jnp.stack([head_re, head_im]), "tm", split_axis=2, concat_axis=3, tiled=True
    )
    spec_re = contract("mcb,kb->mck", turned[0], table_re) - contract(
        "mcb,kb->mck", turned[1], table_im
    )
    spec_im = contract("mcb,kb->mck", turned[1], table_re) + contract(
        "mcb,kb->mck", turned[0], table_im
    )
    rows_local = turned.shape[2]
    first_index = tm_index * rows_local + lax.iota(jnp.int32, rows_local)
    wave = first_index[:, None] + radix_size * row_position[None, :]
    signed = jnp.where(wave < total_time // 2, wave, wave - total_time)
    frequency = signed.astype(jnp.float32) / (total_time / 2)
    angle = phase_of(
        beta[0][:, None, None], beta[1][:, None, None], beta[2][:, None, None], frequency[None]
    )
    spec_re, spec_im = rotate(spec_re, spec_im, angle)
    back_re = contract("mck,kb->mcb", spec_re, table_re) + contract(
        "mck,kb->mcb", spec_im, table_im
    )
    back_im = contract("mck,kb->mcb", spec_im, table_re) - contract(
        "mck,kb->mcb", spec_re, table_im
    )
    untwist = (
        2.0
        * math.pi
        / total_time
        * (first_index[:, None] * row_position[None, :] % total_time).astype(jnp.float32)
    )
    back_re, back_im = rotate(back_re, back_im, untwist[None])
    gathered = lax.all_to_all(
        jnp.stack([back_re, back_im]), "tm", split_axis=3, concat_axis=2, tiled=True
    )
    scale = 1.0 / total_time
    out_re = (
        contract("ka,mkb->mab", table_re, gathered[0])
        + contract("ka,mkb->mab", table_im, gathered[1])
    ) * scale
    out_im = (
        contract("ka,mkb->mab", table_re, gathered[1])
        - contract("ka,mkb->mab", table_im, gathered[0])
    ) * scale
    return jnp.stack([out_re, out_im])


def kerr_term(fields, quartets, intersections):
    count = quartets.shape[1]
    block_size = min(512, count)
    blocks = count // block_size
    grouped = quartets.reshape(4, blocks, block_size).transpose(1, 0, 2)
    weights = intersections.reshape(blocks, block_size)
    modes_all = fields.shape[1]
    mode_ids = lax.iota(jnp.int32, modes_all)

    def accumulate(running, block_item):
        indices, weight = block_item
        out_re, out_im = triple_product(
            jnp.take(fields, indices[1], axis=1),
            jnp.take(fields, indices[2], axis=1),
            jnp.take(fields, indices[3], axis=1),
        )
        owner = (indices[0][None, :] == mode_ids[:, None]).astype(jnp.float32) * weight[None, :]
        add_re = contract("pq,qt->pt", owner, -out_im)
        add_im = contract("pq,qt->pt", owner, out_re)
        return (running + jnp.stack([add_re, add_im]), None)

    running, unused = lax.scan(accumulate, jnp.zeros_like(fields), (grouped, weights))
    return running


def kerr_step(flat, quartets, intersections):
    spread = lax.all_to_all(flat, "mode", split_axis=2, concat_axis=1, tiled=True)
    first = kerr_term(spread, quartets, intersections)
    second = kerr_term(spread + first, quartets, intersections)
    updated = spread + 0.5 * (first + second)
    estimate = 0.5 * (second - first)
    returned, estimate_home = (
        lax.all_to_all(updated, "mode", split_axis=1, concat_axis=2, tiled=True),
        lax.all_to_all(estimate, "mode", split_axis=1, concat_axis=2, tiled=True),
    )
    error_part = jnp.sum(estimate_home * estimate_home, axis=(0, 2))
    field_part = jnp.sum(returned * returned, axis=(0, 2))
    return (returned, error_part, field_part)


def shards_general(field, beta, quartets, intersections):
    modes_local = field.shape[1]
    time_local = field.shape[2]
    table_re, table_im = dft_tables(RADIX)
    state = field.reshape(2, modes_local, time_local // RADIX, RADIX)
    state = to_columns(state)
    error_rows = []
    for step_index in range(STEPS):
        columns = state
        columns = linear_step(columns, beta, table_re, table_im)
        updated, error_part, field_part = kerr_step(
            columns.reshape(2, modes_local, time_local), quartets, intersections
        )
        error_sq, field_sq = lax.psum((error_part, field_part), "tm")
        error_rows.append(jnp.sqrt(error_sq / (field_sq + epsilon)))
        state = updated.reshape(columns.shape)
    state = to_rows(state)
    errors = jnp.stack(error_rows)
    return (state.reshape(2, modes_local, time_local), errors)


UNROLL = 8


def split(value):
    high = value.astype(jnp.bfloat16)
    low = (value - high.astype(jnp.float32)).astype(jnp.bfloat16)
    return high, low


def split_table(value):
    high = lax.reduce_precision(value, exponent_bits=8, mantissa_bits=7)
    return high.astype(jnp.bfloat16), (value - high).astype(jnp.bfloat16)


def product(left, right):
    dot = lambda a, b: jnp.dot(a, b, preferred_element_type=jnp.float32)
    return dot(left[0], right[0]) + (dot(left[0], right[1]) + dot(left[1], right[0]))


def spectral_kernel(x_ref, m1h, m1l, m2h, m2l, twist_ref, rotor_ref, out_ref):
    radix = twist_ref.shape[1]
    m1 = (m1h[...], m1l[...])
    m2 = (m2h[...], m2l[...])
    real = x_ref[:, 0, 0].reshape(radix, radix)
    imag = x_ref[:, 1, 0].reshape(radix, radix)
    head = product(m1, split(jnp.concatenate([real, imag], axis=0)))
    head_re, head_im = head[:radix], head[radix:]
    tw_re, tw_im = twist_ref[0], twist_ref[1]
    re = head_re * tw_re - head_im * tw_im
    im = head_re * tw_im + head_im * tw_re
    spec = product(split(jnp.concatenate([re, im], axis=1)), m2)
    spec_re, spec_im = spec[:, :radix], spec[:, radix:]
    ro_re, ro_im = rotor_ref[0, 0], rotor_ref[1, 0]
    re = spec_re * ro_re - spec_im * ro_im
    im = spec_re * ro_im + spec_im * ro_re
    back = product(split(jnp.concatenate([re, im], axis=1)), m1)
    back_re, back_im = back[:, :radix], back[:, radix:]
    re = back_re * tw_re + back_im * tw_im
    im = back_im * tw_re - back_re * tw_im
    out = product(m2, split(jnp.concatenate([re, im], axis=0)))
    shape = out_ref.shape[:1] + out_ref.shape[3:]
    out_ref[:, 0, 0] = out[:radix].reshape(shape)
    out_ref[:, 1, 0] = out[radix:].reshape(shape)


def spectral(x, tables, twist, rotor, blocks):
    count, _, modes, rows, radix = x.shape
    whole = lambda a: pl.BlockSpec(a.shape, lambda g: (0,) * a.ndim)
    return pl.pallas_call(
        spectral_kernel,
        grid=(modes,),
        in_specs=[pl.BlockSpec((count, 2, 1, rows, radix), lambda g: (0, 0, g, 0, 0))]
        + [whole(t) for t in tables]
        + [whole(twist), pl.BlockSpec((2, 1, radix, radix), lambda g: (0, g, 0, 0))],
        out_specs=pl.BlockSpec((blocks, 2, 1, radix // blocks, radix), lambda g: (0, 0, g, 0, 0)),
        out_shape=jax.ShapeDtypeStruct((blocks, 2, modes, radix // blocks, radix), jnp.float32),
        compiler_params=pltpu.CompilerParams(vmem_limit_bytes=48 * 1024 * 1024),
        name="spectral",
    )(x, *tables, twist, rotor)


def kerr_kernel(stride, quartets, weights, lin_ref, out_ref, err_ref, first_ref, acc_ref, mid_ref):
    count = quartets.shape[1]
    unroll = UNROLL if count % UNROLL == 0 else 1

    def evaluate(src, dst):
        dst[...] = jnp.zeros_like(dst)

        def chunk(c, carry):
            pending = []
            for u in range(unroll):
                q = c * unroll + u
                l, m, n = quartets[1, q], quartets[2, q], quartets[3, q]
                w = weights[q]
                re, im = triple_product(
                    (src[l], src[l + stride]), (src[m], src[m + stride]), (src[n], src[n + stride])
                )
                pending.append((quartets[0, q], -w * im, w * re))
            for p, re, im in pending:
                dst[p] += re
                dst[p + stride] += im
            return carry

        lax.fori_loop(0, count // unroll, chunk, 0)

    evaluate(lin_ref, first_ref)
    mid_ref[...] = lin_ref[...] + first_ref[...]
    evaluate(mid_ref, acc_ref)

    def finish(i, carry):
        first, second = first_ref[i], acc_ref[i]
        new = lin_ref[i] + 0.5 * (first + second)
        estimate = 0.5 * (second - first)
        out_ref[i] = new
        err_ref[0, pl.ds(i, 1)] = jnp.sum(estimate * estimate, axis=0, keepdims=True)
        err_ref[1, pl.ds(i, 1)] = jnp.sum(new * new, axis=0, keepdims=True)
        return carry

    lax.fori_loop(0, lin_ref.shape[0], finish, 0, unroll=4)


def kerr(lin, quartets, weights, stride):
    planes, rows, lanes = lin.shape
    vmem = pl.BlockSpec(memory_space=pltpu.VMEM)
    smem = pl.BlockSpec(memory_space=pltpu.SMEM)
    return pl.pallas_call(
        functools.partial(kerr_kernel, stride),
        in_specs=[smem, smem, vmem],
        out_specs=[vmem, vmem],
        out_shape=[
            jax.ShapeDtypeStruct(lin.shape, jnp.float32),
            jax.ShapeDtypeStruct((2, planes, lanes), jnp.float32),
        ],
        scratch_shapes=[pltpu.VMEM(lin.shape, jnp.float32)] * 3,
        compiler_params=pltpu.CompilerParams(vmem_limit_bytes=40 * 1024 * 1024),
        name="kerr",
    )(quartets, weights, lin)


def shards(ways, field, beta, quartets, intersections):
    mode_ways, tm_ways = ways
    devices = mode_ways * tm_ways
    _, modes_local, time_local = field.shape
    total_time = time_local * tm_ways
    radix = math.isqrt(total_time)
    own = modes_local // tm_ways
    modes_all = modes_local * mode_ways
    rows = radix // devices
    tm_index = lax.axis_index("tm")
    mode_index = lax.axis_index("mode")

    table_re, table_im = dft_tables(radix)
    m1 = jnp.concatenate(
        [jnp.concatenate([table_re, -table_im], 1), jnp.concatenate([table_im, table_re], 1)], 0
    )
    m2 = jnp.concatenate(
        [jnp.concatenate([table_re, table_im], 1), jnp.concatenate([-table_im, table_re], 1)], 0
    )
    tables = split_table(m1) + split_table(m2)
    position = lax.iota(jnp.int32, radix)
    angle = (
        -2.0
        * math.pi
        / total_time
        * (position[:, None] * position[None, :] % total_time).astype(jnp.float32)
    )
    twist = jnp.stack([jnp.cos(angle), jnp.sin(angle)])
    wave = position[:, None] + radix * position[None, :]
    signed = jnp.where(wave < total_time // 2, wave, wave - total_time)
    frequency = signed.astype(jnp.float32) / (total_time / 2)
    mine = lax.dynamic_slice_in_dim(beta, tm_index * own, own, axis=1)
    phase = phase_of(
        mine[0][:, None, None], mine[1][:, None, None], mine[2][:, None, None], frequency[None]
    )
    rotor = jnp.stack([jnp.cos(phase), jnp.sin(phase)]) * (1.0 / total_time)

    holder = quartets % modes_local // own * mode_ways + quartets // modes_local
    planes = holder * (2 * own) + quartets % own

    state = field.reshape(2, tm_ways, own, time_local // radix, radix).transpose(1, 0, 2, 3, 4)
    state = lax.all_to_all(state, "tm", split_axis=0, concat_axis=0, tiled=True)
    sums = []
    for step_index in range(STEPS):
        state = spectral(state, tables, twist, rotor, devices)
        state = lax.all_to_all(state, ("tm", "mode"), split_axis=0, concat_axis=0, tiled=True)
        flat, part = kerr(
            state.reshape(2 * modes_all, rows, radix), planes, intersections, own
        )
        sums.append(part)
        state = flat.reshape(devices, 2, own, rows, radix)
        if step_index < STEPS - 1:
            state = lax.all_to_all(state, ("tm", "mode"), split_axis=0, concat_axis=0, tiled=True)
    state = state.reshape(tm_ways, mode_ways, 2, own, rows, radix)
    state = lax.all_to_all(state, "mode", split_axis=1, concat_axis=1, tiled=True)
    out = state.transpose(2, 0, 3, 1, 4, 5).reshape(2, modes_local, time_local)

    norms = jnp.sum(jnp.stack(sums), axis=-1).reshape(STEPS, 2, tm_ways, mode_ways, 2, own)
    norms = jnp.sum(norms, axis=4)
    norms = lax.psum(norms, ("mode", "tm"))
    norms = lax.dynamic_index_in_dim(norms, mode_index, axis=3, keepdims=False)
    norms = norms.reshape(STEPS, 2, modes_local)
    errors = jnp.sqrt(norms[:, 0] / (norms[:, 1] + epsilon))
    return (out, errors)


def solution(mesh):
    placed = (P(None, "mode", "tm"), P(None, "mode"), P(), P())

    def body(field, beta, quartets, intersections):
        mode_ways, tm_ways = mesh.shape["mode"], mesh.shape["tm"]
        devices = mode_ways * tm_ways
        if field.shape[1] % tm_ways == 0 and RADIX % (8 * devices) == 0:
            return shards((mode_ways, tm_ways), field, beta, quartets, intersections)
        return shards_general(field, beta, quartets, intersections)

    return jax.shard_map(
        body,
        mesh=mesh,
        in_specs=placed,
        out_specs=(P(None, "mode", "tm"), P(None, "mode")),
        check_vma=False,
    )
```

```python
import functools
import math

import jax
import jax.numpy as jnp
from jax import lax
from jax.experimental import pallas as pl
from jax.experimental.pallas import tpu as pltpu
from jax.sharding import PartitionSpec as P

RADIX = 256
STEPS = 2


epsilon = 1e-06


def phase_of(offset, slope, curve, frequency):
    return math.pi * offset + 300.0 * slope * frequency + 3000.0 * curve * frequency * frequency


def triple_product(left_field, middle_field, conj_field):
    prod_re = left_field[0] * middle_field[0] - left_field[1] * middle_field[1]
    prod_im = left_field[0] * middle_field[1] + left_field[1] * middle_field[0]
    out_re = prod_re * conj_field[0] + prod_im * conj_field[1]
    out_im = prod_im * conj_field[0] - prod_re * conj_field[1]
    return (out_re, out_im)


def contract(form, first_operand, second_operand):
    return jnp.einsum(form, first_operand, second_operand, precision=lax.Precision.HIGHEST)


def rotate(real_part, imag_part, angle):
    cosine = jnp.cos(angle)
    sine_part = jnp.sin(angle)
    return (real_part * cosine - imag_part * sine_part, real_part * sine_part + imag_part * cosine)


def dft_tables(length):
    positions = lax.iota(jnp.int32, length)
    product = positions[:, None] * positions[None, :] % length
    angle = -2.0 * math.pi / length * product.astype(jnp.float32)
    return (jnp.cos(angle), jnp.sin(angle))


def to_columns(state):
    return lax.all_to_all(state, "tm", split_axis=3, concat_axis=2, tiled=True)


def to_rows(state):
    return lax.all_to_all(state, "tm", split_axis=2, concat_axis=3, tiled=True)


def linear_step(state, beta, table_re, table_im):
    radix_size = table_re.shape[0]
    total_time = radix_size * radix_size
    cols_local = state.shape[3]
    tm_index = lax.axis_index("tm")
    head_re = contract("ka,mab->mkb", table_re, state[0]) - contract(
        "ka,mab->mkb", table_im, state[1]
    )
    head_im = contract("ka,mab->mkb", table_re, state[1]) + contract(
        "ka,mab->mkb", table_im, state[0]
    )
    column = tm_index * cols_local + lax.iota(jnp.int32, cols_local)
    row_position = lax.iota(jnp.int32, radix_size)
    twist = (
        -2.0
        * math.pi
        / total_time
        * (row_position[:, None] * column[None, :] % total_time).astype(jnp.float32)
    )
    head_re, head_im = rotate(head_re, head_im, twist[None])
    turned = lax.all_to_all(
        jnp.stack([head_re, head_im]), "tm", split_axis=2, concat_axis=3, tiled=True
    )
    spec_re = contract("mcb,kb->mck", turned[0], table_re) - contract(
        "mcb,kb->mck", turned[1], table_im
    )
    spec_im = contract("mcb,kb->mck", turned[1], table_re) + contract(
        "mcb,kb->mck", turned[0], table_im
    )
    rows_local = turned.shape[2]
    first_index = tm_index * rows_local + lax.iota(jnp.int32, rows_local)
    wave = first_index[:, None] + radix_size * row_position[None, :]
    signed = jnp.where(wave < total_time // 2, wave, wave - total_time)
    frequency = signed.astype(jnp.float32) / (total_time / 2)
    angle = phase_of(
        beta[0][:, None, None], beta[1][:, None, None], beta[2][:, None, None], frequency[None]
    )
    spec_re, spec_im = rotate(spec_re, spec_im, angle)
    back_re = contract("mck,kb->mcb", spec_re, table_re) + contract(
        "mck,kb->mcb", spec_im, table_im
    )
    back_im = contract("mck,kb->mcb", spec_im, table_re) - contract(
        "mck,kb->mcb", spec_re, table_im
    )
    untwist = (
        2.0
        * math.pi
        / total_time
        * (first_index[:, None] * row_position[None, :] % total_time).astype(jnp.float32)
    )
    back_re, back_im = rotate(back_re, back_im, untwist[None])
    gathered = lax.all_to_all(
        jnp.stack([back_re, back_im]), "tm", split_axis=3, concat_axis=2, tiled=True
    )
    scale = 1.0 / total_time
    out_re = (
        contract("ka,mkb->mab", table_re, gathered[0])
        + contract("ka,mkb->mab", table_im, gathered[1])
    ) * scale
    out_im = (
        contract("ka,mkb->mab", table_re, gathered[1])
        - contract("ka,mkb->mab", table_im, gathered[0])
    ) * scale
    return jnp.stack([out_re, out_im])


def kerr_term(fields, quartets, intersections):
    count = quartets.shape[1]
    block_size = min(512, count)
    blocks = count // block_size
    grouped = quartets.reshape(4, blocks, block_size).transpose(1, 0, 2)
    weights = intersections.reshape(blocks, block_size)
    modes_all = fields.shape[1]
    mode_ids = lax.iota(jnp.int32, modes_all)

    def accumulate(running, block_item):
        indices, weight = block_item
        out_re, out_im = triple_product(
            jnp.take(fields, indices[1], axis=1),
            jnp.take(fields, indices[2], axis=1),
            jnp.take(fields, indices[3], axis=1),
        )
        owner = (indices[0][None, :] == mode_ids[:, None]).astype(jnp.float32) * weight[None, :]
        add_re = contract("pq,qt->pt", owner, -out_im)
        add_im = contract("pq,qt->pt", owner, out_re)
        return (running + jnp.stack([add_re, add_im]), None)

    running, unused = lax.scan(accumulate, jnp.zeros_like(fields), (grouped, weights))
    return running


def kerr_step(flat, quartets, intersections):
    spread = lax.all_to_all(flat, "mode", split_axis=2, concat_axis=1, tiled=True)
    first = kerr_term(spread, quartets, intersections)
    second = kerr_term(spread + first, quartets, intersections)
    updated = spread + 0.5 * (first + second)
    estimate = 0.5 * (second - first)
    returned, estimate_home = (
        lax.all_to_all(updated, "mode", split_axis=1, concat_axis=2, tiled=True),
        lax.all_to_all(estimate, "mode", split_axis=1, concat_axis=2, tiled=True),
    )
    error_part = jnp.sum(estimate_home * estimate_home, axis=(0, 2))
    field_part = jnp.sum(returned * returned, axis=(0, 2))
    return (returned, error_part, field_part)


def shards_general(field, beta, quartets, intersections):
    modes_local = field.shape[1]
    time_local = field.shape[2]
    table_re, table_im = dft_tables(RADIX)
    state = field.reshape(2, modes_local, time_local // RADIX, RADIX)
    state = to_columns(state)
    error_rows = []
    for step_index in range(STEPS):
        columns = state
        columns = linear_step(columns, beta, table_re, table_im)
        updated, error_part, field_part = kerr_step(
            columns.reshape(2, modes_local, time_local), quartets, intersections
        )
        error_sq, field_sq = lax.psum((error_part, field_part), "tm")
        error_rows.append(jnp.sqrt(error_sq / (field_sq + epsilon)))
        state = updated.reshape(columns.shape)
    state = to_rows(state)
    errors = jnp.stack(error_rows)
    return (state.reshape(2, modes_local, time_local), errors)


UNROLL = 8
CHAINS = 1


def split(value):
    high = value.astype(jnp.bfloat16)
    low = (value - high.astype(jnp.float32)).astype(jnp.bfloat16)
    return high, low


def split_table(value):
    high = lax.reduce_precision(value, exponent_bits=8, mantissa_bits=7)
    return high.astype(jnp.bfloat16), (value - high).astype(jnp.bfloat16)


def product(left, right):
    dot = lambda a, b: jnp.dot(a, b, preferred_element_type=jnp.float32)
    return dot(left[0], right[0]) + (dot(left[0], right[1]) + dot(left[1], right[0]))


def spectral_kernel(x_ref, m1h, m1l, m2h, m2l, twist_ref, rotor_ref, out_ref):
    radix = twist_ref.shape[1]
    m1 = (m1h[...], m1l[...])
    m2 = (m2h[...], m2l[...])
    real = x_ref[:, 0, 0].reshape(radix, radix)
    imag = x_ref[:, 1, 0].reshape(radix, radix)
    head = product(m1, split(jnp.concatenate([real, imag], axis=0)))
    head_re, head_im = head[:radix], head[radix:]
    tw_re, tw_im = twist_ref[0], twist_ref[1]
    re = head_re * tw_re - head_im * tw_im
    im = head_re * tw_im + head_im * tw_re
    spec = product(split(jnp.concatenate([re, im], axis=1)), m2)
    spec_re, spec_im = spec[:, :radix], spec[:, radix:]
    ro_re, ro_im = rotor_ref[0, 0], rotor_ref[1, 0]
    re = spec_re * ro_re - spec_im * ro_im
    im = spec_re * ro_im + spec_im * ro_re
    back = product(split(jnp.concatenate([re, im], axis=1)), m1)
    back_re, back_im = back[:, :radix], back[:, radix:]
    re = back_re * tw_re + back_im * tw_im
    im = back_im * tw_re - back_re * tw_im
    out = product(m2, split(jnp.concatenate([re, im], axis=0)))
    shape = out_ref.shape[:1] + out_ref.shape[3:]
    out_ref[:, 0, 0] = out[:radix].reshape(shape)
    out_ref[:, 1, 0] = out[radix:].reshape(shape)


def spectral(x, tables, twist, rotor, blocks):
    count, _, modes, rows, radix = x.shape
    whole = lambda a: pl.BlockSpec(a.shape, lambda g: (0,) * a.ndim)
    return pl.pallas_call(
        spectral_kernel,
        grid=(modes,),
        in_specs=[pl.BlockSpec((count, 2, 1, rows, radix), lambda g: (0, 0, g, 0, 0))]
        + [whole(t) for t in tables]
        + [whole(twist), pl.BlockSpec((2, 1, radix, radix), lambda g: (0, g, 0, 0))],
        out_specs=pl.BlockSpec((blocks, 2, 1, radix // blocks, radix), lambda g: (0, 0, g, 0, 0)),
        out_shape=jax.ShapeDtypeStruct((blocks, 2, modes, radix // blocks, radix), jnp.float32),
        compiler_params=pltpu.CompilerParams(vmem_limit_bytes=48 * 1024 * 1024),
        name="spectral",
    )(x, *tables, twist, rotor)


def kerr_kernel(stride, quartets, weights, lin_ref, out_ref, err_ref, mid_ref, *accs):
    chains = len(accs) // 2
    count = weights.shape[0]
    unroll = UNROLL if count % UNROLL == 0 else 1

    def evaluate(src, totals):
        for total in totals:
            total[...] = jnp.zeros_like(total)

        def chunk(c, carry):
            pending = []
            for u in range(unroll):
                q = c * unroll + u
                l, m, n = quartets[4 * q + 1], quartets[4 * q + 2], quartets[4 * q + 3]
                w = weights[q]
                re, im = triple_product(
                    (src[l], src[l + stride]), (src[m], src[m + stride]), (src[n], src[n + stride])
                )
                pending.append((quartets[4 * q], -w * im, w * re))
            for u, (p, re, im) in enumerate(pending):
                total = totals[u % chains]
                total[p] += re
                total[p + stride] += im
            return carry

        lax.fori_loop(0, count // unroll, chunk, 0)

    evaluate(lin_ref, accs[:chains])
    first_ref = accs[0]

    def combine(i, carry):
        first_ref[i] = sum(total[i] for total in accs[:chains])
        mid_ref[i] = lin_ref[i] + first_ref[i]
        return carry

    lax.fori_loop(0, lin_ref.shape[0], combine, 0, unroll=4)
    evaluate(mid_ref, accs[chains:])

    def finish(i, carry):
        first, second = first_ref[i], sum(total[i] for total in accs[chains:])
        new = lin_ref[i] + 0.5 * (first + second)
        estimate = 0.5 * (second - first)
        out_ref[i] = new
        err_ref[0, pl.ds(i, 1)] = jnp.sum(estimate * estimate, axis=0, keepdims=True)
        err_ref[1, pl.ds(i, 1)] = jnp.sum(new * new, axis=0, keepdims=True)
        return carry

    lax.fori_loop(0, lin_ref.shape[0], finish, 0, unroll=4)


def kerr(lin, quartets, weights, stride):
    planes, rows, lanes = lin.shape
    vmem = pl.BlockSpec(memory_space=pltpu.VMEM)
    smem = pl.BlockSpec(memory_space=pltpu.SMEM)
    return pl.pallas_call(
        functools.partial(kerr_kernel, stride),
        in_specs=[smem, smem, vmem],
        out_specs=[vmem, vmem],
        out_shape=[
            jax.ShapeDtypeStruct(lin.shape, jnp.float32),
            jax.ShapeDtypeStruct((2, planes, lanes), jnp.float32),
        ],
        scratch_shapes=[pltpu.VMEM(lin.shape, jnp.float32)] * (1 + 2 * CHAINS),
        compiler_params=pltpu.CompilerParams(vmem_limit_bytes=40 * 1024 * 1024),
        name="kerr",
    )(quartets, weights, lin)


def shards(ways, field, beta, quartets, intersections):
    mode_ways, tm_ways = ways
    devices = mode_ways * tm_ways
    _, modes_local, time_local = field.shape
    total_time = time_local * tm_ways
    radix = math.isqrt(total_time)
    own = modes_local // tm_ways
    modes_all = modes_local * mode_ways
    rows = radix // devices
    tm_index = lax.axis_index("tm")

    table_re, table_im = dft_tables(radix)
    m1 = jnp.concatenate(
        [jnp.concatenate([table_re, -table_im], 1), jnp.concatenate([table_im, table_re], 1)], 0
    )
    m2 = jnp.concatenate(
        [jnp.concatenate([table_re, table_im], 1), jnp.concatenate([-table_im, table_re], 1)], 0
    )
    tables = split_table(m1) + split_table(m2)
    position = lax.iota(jnp.int32, radix)
    angle = (
        -2.0
        * math.pi
        / total_time
        * (position[:, None] * position[None, :] % total_time).astype(jnp.float32)
    )
    twist = jnp.stack([jnp.cos(angle), jnp.sin(angle)])
    wave = position[:, None] + radix * position[None, :]
    signed = jnp.where(wave < total_time // 2, wave, wave - total_time)
    frequency = signed.astype(jnp.float32) / (total_time / 2)
    mine = lax.dynamic_slice_in_dim(beta, tm_index * own, own, axis=1)
    phase = phase_of(
        mine[0][:, None, None], mine[1][:, None, None], mine[2][:, None, None], frequency[None]
    )
    rotor = jnp.stack([jnp.cos(phase), jnp.sin(phase)]) * (1.0 / total_time)

    holder = quartets % modes_local // own * mode_ways + quartets // modes_local
    planes = (holder * (2 * own) + quartets % own).T.reshape(-1)

    state = field.reshape(2, tm_ways, own, time_local // radix, radix).transpose(1, 0, 2, 3, 4)
    state = lax.all_to_all(state, "tm", split_axis=0, concat_axis=0, tiled=True)
    sums = []
    for step_index in range(STEPS):
        state = spectral(state, tables, twist, rotor, devices)
        state = lax.all_to_all(state, ("tm", "mode"), split_axis=0, concat_axis=0, tiled=True)
        flat, part = kerr(
            state.reshape(2 * modes_all, rows, radix), planes, intersections, own
        )
        sums.append(part)
        state = flat.reshape(devices, 2, own, rows, radix)
        if step_index < STEPS - 1:
            state = lax.all_to_all(state, ("tm", "mode"), split_axis=0, concat_axis=0, tiled=True)
    state = state.reshape(tm_ways, mode_ways, 2, own, rows, radix)
    state = lax.all_to_all(state, "mode", split_axis=1, concat_axis=1, tiled=True)
    out = state.transpose(2, 0, 3, 1, 4, 5).reshape(2, modes_local, time_local)

    norms = jnp.sum(jnp.stack(sums), axis=-1).reshape(STEPS, 2, tm_ways, mode_ways, 2, own)
    norms = jnp.sum(norms, axis=4).transpose(3, 0, 1, 2, 4).reshape(mode_ways, -1)
    norms = jnp.broadcast_to(norms[:, None], (mode_ways, tm_ways, norms.shape[1]))
    norms = norms.reshape(devices, 1, -1)
    norms = lax.all_to_all(norms, ("mode", "tm"), split_axis=0, concat_axis=0, tiled=True)
    norms = jnp.sum(norms, axis=0).reshape(STEPS, 2, modes_local)
    errors = jnp.sqrt(norms[:, 0] / (norms[:, 1] + epsilon))
    return (out, errors)


def solution(mesh):
    placed = (P(None, "mode", "tm"), P(None, "mode"), P(), P())

    def body(field, beta, quartets, intersections):
        mode_ways, tm_ways = mesh.shape["mode"], mesh.shape["tm"]
        devices = mode_ways * tm_ways
        if field.shape[1] % tm_ways == 0 and RADIX % (8 * devices) == 0:
            return shards((mode_ways, tm_ways), field, beta, quartets, intersections)
        return shards_general(field, beta, quartets, intersections)

    return jax.shard_map(
        body,
        mesh=mesh,
        in_specs=placed,
        out_specs=(P(None, "mode", "tm"), P(None, "mode")),
        check_vma=False,
    )
```
